32 devices in a mesh: blk: 8 (over y, x, core), sub: 4 (over z).
Axes of the slice: x: 2, y: 2, z: 4, core: 2. Of those that a mesh axis runs over, the one named last changes fastest.
Arguments:
- flow_state: float32 [6, 64, 8, 512], P(None, 'blk', None, 'sub'), may hold values from -6 to 6
- timestep: float32 [64, 8, 512], P('blk', None, 'sub'), may hold values from 0.05 to 0.3
- coupling: float32 [3, 6, 6], replicated, may hold values from -2.5 to 2.5
- face_type: int32 [8, 2], P('blk'), may hold values from 0 to 3
- face_rot: int32 [8, 2], P('blk'), may hold values from 0 to 3
Outputs:
- updated: float32 [6, 64, 8, 512], P(None, 'blk', None, 'sub')
- fine_residual: float32 [6, 64, 8, 512], P(None, 'blk', None, 'sub')
The draws below stay inside these ranges and needn't reach their ends.
All inputs are finite; a program needn't handle non-finite values.
Results may differ from the reference program's by a relative error of at most 0.0003.
Values sent between devices are 32-bit elements; how exact they have to be, the bound alone decides.
A program may use at most 64 MiB of HBM per device.

```python
import math
import jax
import jax.numpy as jnp
from jax import lax

VARS = 6
CJ = 8
BLOCKS = 8
NI = 64
NK = 512


def with_ends(entries, own_key, low, high):
    longest = entries.shape.index(max(entries.shape))
    spots = []
    for shift in (0, 1):
        where = [jax.random.randint(jax.random.fold_in(own_key, axis), (), 0, length) for axis, length in enumerate(entries.shape)]
        where[longest] = (where[longest] + shift) % entries.shape[longest]
        spots.append(tuple(where))
    return entries.at[spots[0]].set(low).at[spots[1]].set(high)


def steps_of(stream_key, shape, pieces, low, top_value):
    level, own = 1.0, jax.random.fold_in(stream_key, 6)
    for position, shards_of in pieces:
        steps = jnp.exp(jax.random.uniform(jax.random.fold_in(own, position), (shards_of,), jnp.float32, low / len(pieces), top_value / len(pieces)))
        level = level * jnp.repeat(steps, shape[position] // shards_of).reshape([-1 if axis == position else 1 for axis in range(len(shape))])
    return level


def centred(own_key, extent, deviation, limit, shards=(), held_as=jnp.bfloat16):
    drawn = jax.random.normal(own_key, extent, jnp.float32) * deviation
    if len(shards) > 0:
        drawn = steps_of(own_key, extent, shards, -0.22, 0.18) * drawn
    return jnp.clip(drawn, min=-limit, max=limit).astype(held_as)


def setup_inputs(seed: int = 0) -> dict:
    seeds = jax.random.split(jax.random.key(seed), 6)
    return {
        "flow_state": centred(seeds[0], (VARS, NI, CJ, NK), 1.0, 6.0, ((1, 8), (3, 4)), jnp.float32),
        "timestep": jnp.clip(jnp.exp(math.log(0.3) - 1.7917595 * jax.random.uniform(seeds[1], (NI, CJ, NK), jnp.float32) ** steps_of(seeds[1], (NI, CJ, NK), ((0, 8), (2, 4)), -0.2, 0.2)), 0.05, 0.3),
        "coupling": centred(seeds[2], (3, VARS, VARS), VARS ** -0.5, 2.5, (), jnp.float32),
        "face_type": with_ends(jax.random.randint(seeds[3], (BLOCKS, 2), 0, 4), jax.random.fold_in(seeds[3], 1), 0, 3).astype(jnp.int32),
        "face_rot": with_ends(jax.random.randint(seeds[4], (BLOCKS, 2), 0, 4), jax.random.fold_in(seeds[4], 1), 0, 3).astype(jnp.int32),
    }


DAMP_TWO = 0.05
DAMP_FOUR = 0.02
SECTION_COEFFS = (0.4, 1.0)
PRECISE = lax.Precision.HIGHEST


def rotate_plane(plane, rot_code):
    flipped = jnp.where(rot_code % 2 == 1, plane[:, :, ::-1, :], plane)
    turned = jnp.stack([flipped[0], flipped[1], -flipped[3], flipped[2], flipped[4], flipped[5]])
    return jnp.where((rot_code // 2) % 2 == 1, turned, flipped)


def mirrored(rows_in, negated):
    sign_row = jnp.where(jnp.arange(6) == negated, -1.0, 1.0).astype(jnp.float32)
    return rows_in * sign_row[:, None, None, None]


def lower_ghosts(block_cells, prev_last, next_first, kind_code, rot_code):
    wall_rows = mirrored(block_cells[:, :2][:, ::-1], 1)
    picked = jnp.where(kind_code == 0, prev_last, jnp.where(kind_code == 1, next_first[:, ::-1], jnp.where(kind_code == 2, wall_rows, jnp.zeros_like(wall_rows))))
    return rotate_plane(picked, rot_code)


def upper_ghosts(block_cells, prev_last, next_first, kind_code, rot_code):
    wall_rows = mirrored(block_cells[:, -2:][:, ::-1], 1)
    picked = jnp.where(kind_code == 0, next_first, jnp.where(kind_code == 1, prev_last[:, ::-1], jnp.where(kind_code == 2, wall_rows, jnp.zeros_like(wall_rows))))
    return rotate_plane(picked, rot_code)


def flux_of(padded, coupling, direction):
    mixed = jnp.einsum('uv,vijk->uijk', coupling[direction], padded, precision=PRECISE)
    return mixed + 0.5 * padded[1 + direction][None] * padded


def divergence(padded, coupling, direction):
    axis_pos = direction + 1
    length = padded.shape[axis_pos] - 4
    fluxes = flux_of(padded, coupling, direction)
    face_count = length + 1

    def cut_axis(array, offset, amount):
        return lax.slice_in_dim(array, offset, offset + amount, axis=axis_pos)

    near_left = cut_axis(padded, 1, face_count)
    near_right = cut_axis(padded, 2, face_count)
    far_left = cut_axis(padded, 0, face_count)
    far_right = cut_axis(padded, 3, face_count)
    face_flux = 0.5 * (cut_axis(fluxes, 1, face_count) + cut_axis(fluxes, 2, face_count)) - DAMP_TWO * (near_right - near_left) + DAMP_FOUR * (far_right - 3.0 * near_right + 3.0 * near_left - far_left)
    return cut_axis(face_flux, 1, length) - cut_axis(face_flux, 0, length)


def cell_residual(along_i, along_k, block_cells, coupling):
    low_j = mirrored(block_cells[:, :, :2][:, :, ::-1], 2)
    high_j = mirrored(block_cells[:, :, -2:][:, :, ::-1], 2)
    along_j = jnp.concatenate([low_j, block_cells, high_j], axis=2)
    return divergence(along_i, coupling, 0) + divergence(along_j, coupling, 1) + divergence(along_k, coupling, 2)


def residual_whole(field_now, coupling, face_type, face_rot):
    blocks_count = face_type.shape[0]
    block_rows = field_now.shape[1] // blocks_count

    def per_block(number):
        row_start = (number * block_rows).astype(jnp.int32)
        block_cells = lax.dynamic_slice_in_dim(field_now, row_start, block_rows, axis=1)
        prev_start = (((number + blocks_count - 1) % blocks_count) * block_rows + block_rows - 2).astype(jnp.int32)
        next_start = (((number + 1) % blocks_count) * block_rows).astype(jnp.int32)
        prev_last = lax.dynamic_slice_in_dim(field_now, prev_start, 2, axis=1)
        next_first = lax.dynamic_slice_in_dim(field_now, next_start, 2, axis=1)
        low_ghost = lower_ghosts(block_cells, prev_last, next_first, face_type[number, 0], face_rot[number, 0])
        high_ghost = upper_ghosts(block_cells, prev_last, next_first, face_type[number, 1], face_rot[number, 1])
        along_i = jnp.concatenate([low_ghost, block_cells, high_ghost], axis=1)
        along_k = jnp.pad(block_cells, ((0, 0), (0, 0), (0, 0), (2, 2)))
        return cell_residual(along_i, along_k, block_cells, coupling)

    stacked = lax.map(per_block, jnp.arange(blocks_count, dtype=jnp.int32))
    shape_of = stacked.shape
    return jnp.transpose(stacked, (1, 0, 2, 3, 4)).reshape(shape_of[1], shape_of[0] * shape_of[2], shape_of[3], shape_of[4])


def restrict(array):
    shape_of = array.shape
    leading = shape_of[:-3]
    reshaped = array.reshape(leading + (shape_of[-3] // 2, 2, shape_of[-2] // 2, 2, shape_of[-1] // 2, 2))
    return reshaped.mean(axis=(-5, -3, -1))


def prolong(array):
    return jnp.repeat(jnp.repeat(jnp.repeat(array, 2, axis=-3), 2, axis=-2), 2, axis=-1)


def reference(flow_state, timestep, coupling, face_type, face_rot):
    fine_state = flow_state
    for section_alpha in SECTION_COEFFS:
        fine_state = flow_state - section_alpha * timestep[None] * residual_whole(fine_state, coupling, face_type, face_rot)
    fine_residual = residual_whole(fine_state, coupling, face_type, face_rot)
    coarse_start = restrict(fine_state)
    coarse_step = restrict(timestep)
    forcing = residual_whole(coarse_start, coupling, face_type, face_rot) - restrict(fine_residual)
    coarse = coarse_start
    for section_alpha in SECTION_COEFFS:
        coarse = coarse_start - section_alpha * coarse_step[None] * (residual_whole(coarse, coupling, face_type, face_rot) - forcing)
    updated = fine_state + prolong(coarse - coarse_start)
    return updated, fine_residual
```

```python
import functools

import jax
import jax.numpy as jnp
from jax import lax
from jax.experimental import pallas as pl
from jax.experimental.pallas import tpu as pltpu
from jax.sharding import PartitionSpec as P

NEAR = -0.13
FAR = 0.02
CENTRE = 0.66
FIRST = 0.4
NV = 6


def kernel(
    nb, ns, coup, ftype, frot, q_hbm, dt_hbm, upd_hbm, res_hbm,
    q0, s1, s2, dt, acc, cacc, racc, rst, res, cs, c1, cst, upd,
    pf_s, pf_r, hf_r, pc_s, pc_r, hc_s, hc_r,
    loc, hs_sem, hr_sem, ks_sem, kr_sem,
):
    rows, nj, nk = dt.shape
    crows = rows // 2
    blk, sub = lax.axis_index("blk"), lax.axis_index("sub")
    nxt, prv = lax.rem(blk + 1, nb), lax.rem(blk + nb - 1, nb)
    right, left = lax.rem(sub + 1, ns), lax.rem(sub + ns - 1, ns)
    has_left, has_right = sub > 0, sub < ns - 1

    load_q = pltpu.make_async_copy(q_hbm, q0.at[:, pl.ds(2, rows)], loc.at[0])
    load_t = pltpu.make_async_copy(dt_hbm, dt, loc.at[1])
    load_q.start()
    load_t.start()

    barrier = pltpu.get_barrier_semaphore()
    pl.semaphore_signal(barrier, inc=1, device_id={"blk": nxt})
    pl.semaphore_signal(barrier, inc=1, device_id={"blk": prv})

    @pl.when(has_left)
    def _():
        pl.semaphore_signal(barrier, inc=1, device_id={"sub": left})

    @pl.when(has_right)
    def _():
        pl.semaphore_signal(barrier, inc=1, device_id={"sub": right})

    shape = (nj, nk)
    jj = lax.broadcasted_iota(jnp.int32, shape, 0)
    kk = lax.broadcasted_iota(jnp.int32, shape, 1)

    def splat(ref, side):
        return jnp.full(shape, ref[0, side], jnp.int32)

    kinds = [splat(ftype, side) for side in (0, 1)]
    rots = [splat(frot, side) for side in (0, 1)]

    def hcoup(d, u, v):
        return 0.5 * coup[d, u, v]

    def half_flux(x, d):
        s = 0.25 * x[1 + d]
        out = []
        for u in range(NV):
            total = s * x[u]
            for v in range(NV):
                total = total + hcoup(d, u, v) * x[v]
            out.append(total)
        return out

    def roll(x, shift, axis):
        return pltpu.roll(x, shift % x.shape[axis], axis)

    def zero_ends(ref, n):
        for v in range(NV):
            for i in (0, 1, n + 2, n + 3):
                ref[v, i] = jnp.zeros(shape, jnp.float32)

    def own_part(ref, out, n, h):
        step = 2
        j3 = lax.broadcasted_iota(jnp.int32, (step, nj, nk), 1)

        def row(t, carry):
            i0 = t * step

            def at(v, off):
                return ref[v, pl.ds(i0 + 2 + off, step)]

            q = [at(v, 0) for v in range(NV)]
            damp, diffs, sides = [], [], []
            ip = [at(v, 1) for v in range(NV)]
            im = [at(v, -1) for v in range(NV)]
            kp = [roll(x, -h, 2) for x in q]
            km = [roll(x, h, 2) for x in q]
            rp = [roll(x, -h, 1) for x in q]
            rm = [roll(x, h, 1) for x in q]
            jp, jm = [], []
            for v in range(NV):
                sign = -1.0 if v == 2 else 1.0
                edge = sign * q[v] if v == 2 else q[v]
                jp.append(jnp.where(j3 >= nj - h, edge, rp[v]))
                jm.append(jnp.where(j3 < h, edge, rm[v]))
                swap_hi = jnp.where(j3 < nj - h, rp[v], rm[v])
                swap_lo = jnp.where(j3 < h, rp[v], rm[v])
                if v == 2:
                    swap_hi, swap_lo = -swap_hi, -swap_lo
                jpp = jnp.where(j3 < nj - 2 * h, roll(q[v], -2 * h, 1), swap_hi)
                jmm = jnp.where(j3 >= 2 * h, roll(q[v], 2 * h, 1), swap_lo)
                near = ((ip[v] + im[v]) + (jp[v] + jm[v])) + (kp[v] + km[v])
                far = ((at(v, 2) + at(v, -2)) + (jpp + jmm)) + (
                    roll(q[v], -2 * h, 2) + roll(q[v], 2 * h, 2)
                )
                damp.append(CENTRE * q[v] + NEAR * near + FAR * far)
            for d, (p, m) in enumerate(((ip, im), (jp, jm), (kp, km))):
                sp, sm = 0.25 * p[1 + d], 0.25 * m[1 + d]
                diff = [p[v] - m[v] for v in range(NV)]
                for u in range(NV):
                    total = sp * p[u] - sm * m[u]
                    for v in range(NV):
                        total = total + hcoup(d, u, v) * diff[v]
                    damp[u] = damp[u] + total
            for u in range(NV):
                out[u, pl.ds(i0, step)] = damp[u]
            return carry

        lax.fori_loop(0, n // step, row, 0)

    def pack(ref, dst, n, h):
        group = kk // (4 * h)
        packed = []
        for v in range(NV):
            p = roll(ref[v, 2], 2 * h, 1)
            for i in range(1, n):
                p = jnp.where(group == i, roll(ref[v, 2 + i], 2 * h + 4 * h * i, 1), p)
            dst[v] = p
            packed.append(p)
        return packed

    def k_edges(low, high, h):
        r = kk % (4 * h)
        near = [jnp.where(r < 2 * h, low[v], high[v]) for v in range(NV)]
        hf = half_flux(near, 2)
        out = []
        for v in range(NV):
            e = jnp.where(r < 2 * h, -hf[v], hf[v]) + NEAR * near[v]
            far = FAR * jnp.where(r < 2 * h, roll(high[v], -2 * h, 1), roll(low[v], 2 * h, 1))
            inner = jnp.where(r < 2 * h, roll(e, -h, 1), roll(e, h, 1))
            out.append(far + jnp.where((r >= h) & (r < 3 * h), inner, 0.0))
        return out

    def k_correction(own, ref, h):
        low = [jnp.where(jnp.full(shape, sub) > 0, ref[0, v], 0.0) for v in range(NV)]
        high = [jnp.where(jnp.full(shape, sub) < ns - 1, ref[1, v], 0.0) for v in range(NV)]
        got = k_edges(low, high, h)
        return [got[v] - own[v] for v in range(NV)]

    def flip(x):
        bit = 1
        while bit < nj:
            x = jnp.where((jj & bit) == 0, roll(x, -bit, 0), roll(x, bit, 0))
            bit *= 2
        return x

    def ghost(side, same, other, own):
        kind, rot = kinds[side], rots[side]
        out = []
        for v in range(NV):
            wall = -own[v] if v == 1 else own[v]
            g = jnp.where(
                kind == 0, same[v], jnp.where(kind == 1, other[v], jnp.where(kind == 2, wall, 0.0))
            )
            out.append(jnp.where((rot & 1) == 1, flip(g), g))
        turn = ((rot >> 1) & 1) == 1
        out[2], out[3] = jnp.where(turn, -out[3], out[2]), jnp.where(turn, out[2], out[3])
        return out

    def i_edges(before, after, ref, n):
        own = lambda i: [ref[v, 2 + i] for v in range(NV)]
        lo_near = ghost(0, before[1], after[0], own(0))
        lo_far = ghost(0, before[0], after[1], own(1))
        hi_near = ghost(1, after[0], before[1], own(n - 1))
        hi_far = ghost(1, after[1], before[0], own(n - 2))
        lo_f, hi_f = half_flux(lo_near, 0), half_flux(hi_near, 0)
        each = range(NV)
        return {
            0: [FAR * lo_far[v] + NEAR * lo_near[v] - lo_f[v] for v in each],
            1: [FAR * lo_near[v] for v in each],
            n - 1: [FAR * hi_far[v] + NEAR * hi_near[v] + hi_f[v] for v in each],
            n - 2: [FAR * hi_near[v] for v in each],
        }

    def finish(out, n, h, kc, edges, then, order):
        mask = (kk < 2 * h) | (kk >= nk - 2 * h)
        for i in order:
            for v in range(NV):
                r = out[v, i] + jnp.where(mask, roll(kc[v], -(2 * h + 4 * h * i), 1), 0.0)
                if i in edges:
                    r = r + edges[i][v]
                then(v, i, r)

    def pair_sum(x):
        x = x + jnp.where((kk & 1) == 0, roll(x, -1, 1), roll(x, 1, 1))
        return x + jnp.where((jj & 1) == 0, roll(x, -1, 0), roll(x, 1, 0))

    def blk_copies(number, to_next, to_prev, dst):
        made = []
        for side, (src, who) in enumerate(((to_next, nxt), (to_prev, prv))):
            made.append(
                pltpu.make_async_remote_copy(
                    src_ref=src, dst_ref=dst.at[side],
                    send_sem=hs_sem.at[number, side], recv_sem=hr_sem.at[number, side],
                    device_id={"blk": who},
                )
            )
        return made

    def sub_copies(number, src, dst):
        made = []
        for side, who in enumerate((right, left)):
            made.append(
                pltpu.make_async_remote_copy(
                    src_ref=src, dst_ref=dst.at[side],
                    send_sem=ks_sem.at[number, side], recv_sem=kr_sem.at[number, side],
                    device_id={"sub": who},
                )
            )
        return made

    def go(copies):
        for c in copies:
            c.start()

    def sub_go(copies):
        pl.when(has_right)(copies[0].start)
        pl.when(has_left)(copies[1].start)

    def got(copies):
        for c in copies:
            c.wait_recv()

    def sub_got(copies):
        pl.when(has_left)(copies[0].wait_recv)
        pl.when(has_right)(copies[1].wait_recv)

    def sent(copies):
        for c in copies:
            c.wait_send()

    def sub_sent(copies):
        pl.when(has_right)(copies[0].wait_send)
        pl.when(has_left)(copies[1].wait_send)

    def fine_halo(number):
        read = lambda side: [[hf_r[number, side, v, r] for v in range(NV)] for r in (0, 1)]
        return read(0), read(1)

    def coarse_halo(number):
        def read(side):
            x = [hc_r[number, side, v] for v in range(NV)]
            even = (jj & 1) == 0
            return [
                [jnp.where(even, y, roll(y, 1, 0)) for y in x],
                [jnp.where(even, roll(y, -1, 0), y) for y in x],
            ]
        return read(0), read(1)

    def coarse_rows(number, ref):
        even = (jj & 1) == 0
        for v in range(NV):
            hc_s[number, 0, v] = jnp.where(even, ref[v, crows], ref[v, crows + 1])
            hc_s[number, 1, v] = jnp.where(even, ref[v, 2], ref[v, 3])

    edge_first = [0, 1, rows - 2, rows - 1] + list(range(2, rows - 2))
    every = []

    zero_ends(q0, rows)
    zero_ends(s1, rows)
    zero_ends(s2, rows)
    zero_ends(cs, crows)
    zero_ends(c1, crows)
    ends = jnp.where(has_left, 0, 1) + jnp.where(has_right, 0, 1)
    pl.semaphore_wait(barrier, 4 - ends)
    h0 = blk_copies(0, q_hbm.at[:, pl.ds(rows - 2, 2)], q_hbm.at[:, pl.ds(0, 2)], hf_r.at[0])
    go(h0)
    load_q.wait()
    load_t.wait()
    own = k_edges(*[pack(q0, pf_s.at[0], rows, 1)] * 2, 1)
    k0 = sub_copies(0, pf_s.at[0], pf_r.at[0])
    sub_go(k0)
    own_part(q0, acc, rows, 1)
    for i in range(crows):
        cst[i] = 0.125 * pair_sum(dt[2 * i] + dt[2 * i + 1])
    sub_got(k0)
    kc = k_correction(own, pf_r.at[0], 1)
    got(h0)
    before, after = fine_halo(0)

    def store1(v, i, r):
        s1[v, 2 + i] = q0[v, 2 + i] - FIRST * dt[i] * r

    finish(acc, rows, 1, kc, i_edges(before, after, q0, rows), store1, edge_first)

    h1 = blk_copies(1, s1.at[:, pl.ds(rows, 2)], s1.at[:, pl.ds(2, 2)], hf_r.at[1])
    go(h1)
    own = k_edges(*[pack(s1, pf_s.at[1], rows, 1)] * 2, 1)
    k1 = sub_copies(1, pf_s.at[1], pf_r.at[1])
    sub_go(k1)
    own_part(s1, acc, rows, 1)
    sub_got(k1)
    kc = k_correction(own, pf_r.at[1], 1)
    got(h1)
    before, after = fine_halo(1)

    def store2(v, i, r):
        s2[v, 2 + i] = q0[v, 2 + i] - dt[i] * r

    finish(acc, rows, 1, kc, i_edges(before, after, s1, rows), store2, edge_first)

    h2 = blk_copies(2, s2.at[:, pl.ds(rows, 2)], s2.at[:, pl.ds(2, 2)], hf_r.at[2])
    go(h2)
    own = k_edges(*[pack(s2, pf_s.at[2], rows, 1)] * 2, 1)
    k2 = sub_copies(2, pf_s.at[2], pf_r.at[2])
    sub_go(k2)
    for v in range(NV):
        for i in range(crows):
            cs[v, 2 + i] = 0.125 * pair_sum(s2[v, 2 + 2 * i] + s2[v, 3 + 2 * i])
    coarse_rows(0, cs)
    h3 = blk_copies(3, hc_s.at[0, 0], hc_s.at[0, 1], hc_r.at[0])
    go(h3)
    own_c = k_edges(*[pack(cs, pc_s.at[0], crows, 2)] * 2, 2)
    k3 = sub_copies(3, pc_s.at[0], pc_r.at[0])
    sub_go(k3)
    own_part(s2, acc, rows, 1)
    sub_got(k2)
    kc = k_correction(own, pf_r.at[2], 1)
    got(h2)
    before, after = fine_halo(2)

    def store3(v, i, r):
        res[v, i] = r

    finish(acc, rows, 1, kc, i_edges(before, after, s2, rows), store3, edge_first)
    for v in range(NV):
        for i in range(crows):
            r = 0.125 * pair_sum(res[v, 2 * i] + res[v, 2 * i + 1])
            rst[v, i] = r
            c1[v, 2 + i] = cs[v, 2 + i] - FIRST * cst[i] * r

    coarse_rows(1, c1)
    h4 = blk_copies(4, hc_s.at[1, 0], hc_s.at[1, 1], hc_r.at[1])
    go(h4)
    own_d = k_edges(*[pack(c1, pc_s.at[1], crows, 2)] * 2, 2)
    k4 = sub_copies(4, pc_s.at[1], pc_r.at[1])
    sub_go(k4)
    out_r = pltpu.make_async_copy(res, res_hbm, loc.at[2])
    out_r.start()
    own_part(cs, cacc, crows, 2)
    sub_got(k3)
    kc = k_correction(own_c, pc_r.at[0], 2)
    got(h3)
    before, after = coarse_halo(0)

    def store4(v, i, r):
        rst[v, i] = r - rst[v, i]

    every_row = list(range(crows))
    finish(cacc, crows, 2, kc, i_edges(before, after, cs, crows), store4, every_row)
    own_part(c1, racc, crows, 2)
    sub_got(k4)
    kc = k_correction(own_d, pc_r.at[1], 2)
    got(h4)
    before, after = coarse_halo(1)

    def store5(v, i, r):
        change = cst[i] * (r - rst[v, i])
        for ii in (2 * i, 2 * i + 1):
            upd[v, ii] = s2[v, 2 + ii] - change

    finish(racc, crows, 2, kc, i_edges(before, after, c1, crows), store5, every_row)
    out_u = pltpu.make_async_copy(upd, upd_hbm, loc.at[3])
    out_u.start()
    for c in (h0, h1, h2, h3, h4):
        sent(c)
    for c in (k0, k1, k2, k3, k4):
        sub_sent(c)
    out_r.wait()
    out_u.wait()


def solution(mesh):
    nb, ns = mesh.shape["blk"], mesh.shape["sub"]

    def body(flow_state, timestep, coupling, face_type, face_rot):
        nv, rows, nj, nk = flow_state.shape
        f32 = jnp.float32
        half = rows // 2
        any_spec = pl.BlockSpec(memory_space=pl.ANY)
        smem = pl.BlockSpec(memory_space=pltpu.SMEM)
        vm = lambda *s: pltpu.VMEM(s + (nj, nk), f32)
        out = jax.ShapeDtypeStruct(flow_state.shape, f32)
        return pl.pallas_call(
            functools.partial(kernel, nb, ns),
            out_shape=(out, out),
            in_specs=[smem, smem, smem, any_spec, any_spec],
            out_specs=(any_spec, any_spec),
            scratch_shapes=[
                vm(nv, rows + 4), vm(nv, rows + 4), vm(nv, rows + 4), vm(rows),
                vm(nv, rows), vm(nv, half), vm(nv, half), vm(nv, half), vm(nv, rows),
                vm(nv, half + 4), vm(nv, half + 4), vm(half), vm(nv, rows),
                vm(3, nv), vm(3, 2, nv), vm(3, 2, nv, 2),
                vm(2, nv), vm(2, 2, nv), vm(2, 2, nv), vm(2, 2, nv),
                pltpu.SemaphoreType.DMA((4,)),
                pltpu.SemaphoreType.DMA((5, 2)), pltpu.SemaphoreType.DMA((5, 2)),
                pltpu.SemaphoreType.DMA((5, 2)), pltpu.SemaphoreType.DMA((5, 2)),
            ],
            compiler_params=pltpu.CompilerParams(collective_id=0, has_side_effects=True),
        )(coupling, face_type, face_rot, flow_state, timestep)

    return jax.shard_map(
        body,
        mesh=mesh,
        in_specs=(
            P(None, "blk", None, "sub"),
            P("blk", None, "sub"),
            P(),
            P("blk", None),
            P("blk", None),
        ),
        out_specs=(P(None, "blk", None, "sub"), P(None, "blk", None, "sub")),
        check_vma=False,
    )
```

```python
import functools

import jax
import jax.numpy as jnp
from jax import lax
from jax.experimental import pallas as pl
from jax.experimental.pallas import tpu as pltpu
from jax.sharding import PartitionSpec as P

NEAR = -0.13
FAR = 0.02
CENTRE = 0.66
FIRST = 0.4
NV = 6


def kernel(
    nb, ns, coup_hbm, ftype_hbm, frot_hbm, q_hbm, dt_hbm, upd, res,
    coup, ftype, frot, q0, s1, s2, dt, acc, cacc, racc, rst, cs, c1, cst,
    pf_s, pf_r, hf_r, pc_s, pc_r, hc_s, hc_r,
    loc, hs_sem, hr_sem, ks_sem, kr_sem,
):
    rows, nj, nk = dt.shape
    crows = rows // 2
    blk, sub = lax.axis_index("blk"), lax.axis_index("sub")
    nxt, prv = lax.rem(blk + 1, nb), lax.rem(blk + nb - 1, nb)
    right, left = lax.rem(sub + 1, ns), lax.rem(sub + ns - 1, ns)
    has_left, has_right = sub > 0, sub < ns - 1

    load_q = pltpu.make_async_copy(q_hbm, q0.at[:, pl.ds(2, rows)], loc.at[0])
    load_t = pltpu.make_async_copy(dt_hbm, dt, loc.at[1])
    loads = [load_q, load_t]
    for n, (src, dst) in enumerate(((coup_hbm, coup), (ftype_hbm, ftype), (frot_hbm, frot))):
        loads.append(pltpu.make_async_copy(src, dst, loc.at[2 + n]))

    barrier = pltpu.get_barrier_semaphore()
    pl.semaphore_signal(barrier, inc=1, device_id={"blk": nxt})
    pl.semaphore_signal(barrier, inc=1, device_id={"blk": prv})

    @pl.when(has_left)
    def _():
        pl.semaphore_signal(barrier, inc=1, device_id={"sub": left})

    @pl.when(has_right)
    def _():
        pl.semaphore_signal(barrier, inc=1, device_id={"sub": right})

    for load in loads:
        load.start()

    shape = (nj, nk)
    jj = lax.broadcasted_iota(jnp.int32, shape, 0)
    kk = lax.broadcasted_iota(jnp.int32, shape, 1)

    def splat(ref, side):
        return jnp.full(shape, ref[0, side], jnp.int32)


    def hcoup(d, u, v):
        return 0.5 * coup[d, u, v]

    def half_flux(x, d):
        s = 0.25 * x[1 + d]
        out = []
        for u in range(NV):
            total = s * x[u]
            for v in range(NV):
                total = total + hcoup(d, u, v) * x[v]
            out.append(total)
        return out

    def roll(x, shift, axis):
        return pltpu.roll(x, shift % x.shape[axis], axis)

    def zero_ends(ref, n):
        for v in range(NV):
            for i in (0, 1, n + 2, n + 3):
                ref[v, i] = jnp.zeros(shape, jnp.float32)

    def own_part(ref, out, n, h):
        step = 2
        j3 = lax.broadcasted_iota(jnp.int32, (step, nj, nk), 1)

        def row(t, carry):
            i0 = t * step

            def at(v, off):
                return ref[v, pl.ds(i0 + 2 + off, step)]

            q = [at(v, 0) for v in range(NV)]
            damp, diffs, sides = [], [], []
            ip = [at(v, 1) for v in range(NV)]
            im = [at(v, -1) for v in range(NV)]
            kp = [roll(x, -h, 2) for x in q]
            km = [roll(x, h, 2) for x in q]
            rp = [roll(x, -h, 1) for x in q]
            rm = [roll(x, h, 1) for x in q]
            jp, jm = [], []
            for v in range(NV):
                sign = -1.0 if v == 2 else 1.0
                edge = sign * q[v] if v == 2 else q[v]
                jp.append(jnp.where(j3 >= nj - h, edge, rp[v]))
                jm.append(jnp.where(j3 < h, edge, rm[v]))
                swap_hi = jnp.where(j3 < nj - h, rp[v], rm[v])
                swap_lo = jnp.where(j3 < h, rp[v], rm[v])
                if v == 2:
                    swap_hi, swap_lo = -swap_hi, -swap_lo
                jpp = jnp.where(j3 < nj - 2 * h, roll(q[v], -2 * h, 1), swap_hi)
                jmm = jnp.where(j3 >= 2 * h, roll(q[v], 2 * h, 1), swap_lo)
                near = ((ip[v] + im[v]) + (jp[v] + jm[v])) + (kp[v] + km[v])
                far = ((at(v, 2) + at(v, -2)) + (jpp + jmm)) + (
                    roll(q[v], -2 * h, 2) + roll(q[v], 2 * h, 2)
                )
                damp.append(CENTRE * q[v] + NEAR * near + FAR * far)
            for d, (p, m) in enumerate(((ip, im), (jp, jm), (kp, km))):
                sp, sm = 0.25 * p[1 + d], 0.25 * m[1 + d]
                diff = [p[v] - m[v] for v in range(NV)]
                for u in range(NV):
                    total = sp * p[u] - sm * m[u]
                    for v in range(NV):
                        total = total + hcoup(d, u, v) * diff[v]
                    damp[u] = damp[u] + total
            for u in range(NV):
                out[u, pl.ds(i0, step)] = damp[u]
            return carry

        lax.fori_loop(0, n // step, row, 0)

    def pack(ref, dst, n, h):
        group = kk // (4 * h)
        packed = []
        for v in range(NV):
            p = roll(ref[v, 2], 2 * h, 1)
            for i in range(1, n):
                p = jnp.where(group == i, roll(ref[v, 2 + i], 2 * h + 4 * h * i, 1), p)
            dst[v] = p
            packed.append(p)
        return packed

    def k_edges(low, high, h):
        r = kk % (4 * h)
        near = [jnp.where(r < 2 * h, low[v], high[v]) for v in range(NV)]
        hf = half_flux(near, 2)
        out = []
        for v in range(NV):
            e = jnp.where(r < 2 * h, -hf[v], hf[v]) + NEAR * near[v]
            far = FAR * jnp.where(r < 2 * h, roll(high[v], -2 * h, 1), roll(low[v], 2 * h, 1))
            inner = jnp.where(r < 2 * h, roll(e, -h, 1), roll(e, h, 1))
            out.append(far + jnp.where((r >= h) & (r < 3 * h), inner, 0.0))
        return out

    def k_correction(own, ref, h):
        low = [jnp.where(jnp.full(shape, sub) > 0, ref[0, v], 0.0) for v in range(NV)]
        high = [jnp.where(jnp.full(shape, sub) < ns - 1, ref[1, v], 0.0) for v in range(NV)]
        got = k_edges(low, high, h)
        return [got[v] - own[v] for v in range(NV)]

    def flip(x):
        bit = 1
        while bit < nj:
            x = jnp.where((jj & bit) == 0, roll(x, -bit, 0), roll(x, bit, 0))
            bit *= 2
        return x

    def ghost(side, same, other, own):
        kind, rot = kinds[side], rots[side]
        out = []
        for v in range(NV):
            wall = -own[v] if v == 1 else own[v]
            g = jnp.where(
                kind == 0, same[v], jnp.where(kind == 1, other[v], jnp.where(kind == 2, wall, 0.0))
            )
            out.append(jnp.where((rot & 1) == 1, flip(g), g))
        turn = ((rot >> 1) & 1) == 1
        out[2], out[3] = jnp.where(turn, -out[3], out[2]), jnp.where(turn, out[2], out[3])
        return out

    def i_edges(before, after, ref, n):
        own = lambda i: [ref[v, 2 + i] for v in range(NV)]
        lo_near = ghost(0, before[1], after[0], own(0))
        lo_far = ghost(0, before[0], after[1], own(1))
        hi_near = ghost(1, after[0], before[1], own(n - 1))
        hi_far = ghost(1, after[1], before[0], own(n - 2))
        lo_f, hi_f = half_flux(lo_near, 0), half_flux(hi_near, 0)
        each = range(NV)
        return {
            0: [FAR * lo_far[v] + NEAR * lo_near[v] - lo_f[v] for v in each],
            1: [FAR * lo_near[v] for v in each],
            n - 1: [FAR * hi_far[v] + NEAR * hi_near[v] + hi_f[v] for v in each],
            n - 2: [FAR * hi_near[v] for v in each],
        }

    def finish(out, n, h, kc, edges, then, order):
        mask = (kk < 2 * h) | (kk >= nk - 2 * h)
        for i in order:
            for v in range(NV):
                r = out[v, i] + jnp.where(mask, roll(kc[v], -(2 * h + 4 * h * i), 1), 0.0)
                if i in edges:
                    r = r + edges[i][v]
                then(v, i, r)

    def pair_sum(x):
        x = x + jnp.where((kk & 1) == 0, roll(x, -1, 1), roll(x, 1, 1))
        return x + jnp.where((jj & 1) == 0, roll(x, -1, 0), roll(x, 1, 0))

    def blk_copies(number, to_next, to_prev, dst):
        made = []
        for side, (src, who) in enumerate(((to_next, nxt), (to_prev, prv))):
            made.append(
                pltpu.make_async_remote_copy(
                    src_ref=src, dst_ref=dst.at[side],
                    send_sem=hs_sem.at[number, side], recv_sem=hr_sem.at[number, side],
                    device_id={"blk": who},
                )
            )
        return made

    def sub_copies(number, src, dst):
        made = []
        for side, who in enumerate((right, left)):
            made.append(
                pltpu.make_async_remote_copy(
                    src_ref=src, dst_ref=dst.at[side],
                    send_sem=ks_sem.at[number, side], recv_sem=kr_sem.at[number, side],
                    device_id={"sub": who},
                )
            )
        return made

    def go(copies):
        for c in copies:
            c.start()

    def sub_go(copies):
        pl.when(has_right)(copies[0].start)
        pl.when(has_left)(copies[1].start)

    def got(copies):
        for c in copies:
            c.wait_recv()

    def sub_got(copies):
        pl.when(has_left)(copies[0].wait_recv)
        pl.when(has_right)(copies[1].wait_recv)

    def sent(copies):
        for c in copies:
            c.wait_send()

    def sub_sent(copies):
        pl.when(has_right)(copies[0].wait_send)
        pl.when(has_left)(copies[1].wait_send)

    def fine_halo(number):
        read = lambda side: [[hf_r[number, side, v, r] for v in range(NV)] for r in (0, 1)]
        return read(0), read(1)

    def coarse_halo(number):
        def read(side):
            x = [hc_r[number, side, v] for v in range(NV)]
            even = (jj & 1) == 0
            return [
                [jnp.where(even, y, roll(y, 1, 0)) for y in x],
                [jnp.where(even, roll(y, -1, 0), y) for y in x],
            ]
        return read(0), read(1)

    def coarse_rows(number, ref):
        even = (jj & 1) == 0
        for v in range(NV):
            hc_s[number, 0, v] = jnp.where(even, ref[v, crows], ref[v, crows + 1])
            hc_s[number, 1, v] = jnp.where(even, ref[v, 2], ref[v, 3])

    edge_first = [0, 1, rows - 2, rows - 1] + list(range(2, rows - 2))
    every = []

    zero_ends(q0, rows)
    zero_ends(s1, rows)
    zero_ends(s2, rows)
    zero_ends(cs, crows)
    zero_ends(c1, crows)
    ends = jnp.where(has_left, 0, 1) + jnp.where(has_right, 0, 1)
    load_q.wait()
    pl.semaphore_wait(barrier, 4 - ends)
    h0 = blk_copies(0, q0.at[:, pl.ds(rows, 2)], q0.at[:, pl.ds(2, 2)], hf_r.at[0])
    go(h0)
    for load in loads[1:]:
        load.wait()
    kinds = [splat(ftype, side) for side in (0, 1)]
    rots = [splat(frot, side) for side in (0, 1)]
    own = k_edges(*[pack(q0, pf_s.at[0], rows, 1)] * 2, 1)
    k0 = sub_copies(0, pf_s.at[0], pf_r.at[0])
    sub_go(k0)
    own_part(q0, acc, rows, 1)
    for i in range(crows):
        cst[i] = 0.125 * pair_sum(dt[2 * i] + dt[2 * i + 1])
    sub_got(k0)
    kc = k_correction(own, pf_r.at[0], 1)
    got(h0)
    before, after = fine_halo(0)

    def store1(v, i, r):
        s1[v, 2 + i] = q0[v, 2 + i] - FIRST * dt[i] * r

    finish(acc, rows, 1, kc, i_edges(before, after, q0, rows), store1, edge_first)

    h1 = blk_copies(1, s1.at[:, pl.ds(rows, 2)], s1.at[:, pl.ds(2, 2)], hf_r.at[1])
    go(h1)
    own = k_edges(*[pack(s1, pf_s.at[1], rows, 1)] * 2, 1)
    k1 = sub_copies(1, pf_s.at[1], pf_r.at[1])
    sub_go(k1)
    own_part(s1, acc, rows, 1)
    sub_got(k1)
    kc = k_correction(own, pf_r.at[1], 1)
    got(h1)
    before, after = fine_halo(1)

    def store2(v, i, r):
        s2[v, 2 + i] = q0[v, 2 + i] - dt[i] * r

    finish(acc, rows, 1, kc, i_edges(before, after, s1, rows), store2, edge_first)

    h2 = blk_copies(2, s2.at[:, pl.ds(rows, 2)], s2.at[:, pl.ds(2, 2)], hf_r.at[2])
    go(h2)
    own = k_edges(*[pack(s2, pf_s.at[2], rows, 1)] * 2, 1)
    k2 = sub_copies(2, pf_s.at[2], pf_r.at[2])
    sub_go(k2)
    for v in range(NV):
        for i in range(crows):
            cs[v, 2 + i] = 0.125 * pair_sum(s2[v, 2 + 2 * i] + s2[v, 3 + 2 * i])
    coarse_rows(0, cs)
    h3 = blk_copies(3, hc_s.at[0, 0], hc_s.at[0, 1], hc_r.at[0])
    go(h3)
    own_c = k_edges(*[pack(cs, pc_s.at[0], crows, 2)] * 2, 2)
    k3 = sub_copies(3, pc_s.at[0], pc_r.at[0])
    sub_go(k3)
    own_part(s2, acc, rows, 1)
    sub_got(k2)
    kc = k_correction(own, pf_r.at[2], 1)
    got(h2)
    before, after = fine_halo(2)

    def store3(v, i, r):
        res[v, i] = r

    finish(acc, rows, 1, kc, i_edges(before, after, s2, rows), store3, edge_first)
    for v in range(NV):
        for i in range(crows):
            r = 0.125 * pair_sum(res[v, 2 * i] + res[v, 2 * i + 1])
            rst[v, i] = r
            c1[v, 2 + i] = cs[v, 2 + i] - FIRST * cst[i] * r

    coarse_rows(1, c1)
    h4 = blk_copies(4, hc_s.at[1, 0], hc_s.at[1, 1], hc_r.at[1])
    go(h4)
    own_d = k_edges(*[pack(c1, pc_s.at[1], crows, 2)] * 2, 2)
    k4 = sub_copies(4, pc_s.at[1], pc_r.at[1])
    sub_go(k4)
    own_part(cs, cacc, crows, 2)
    sub_got(k3)
    kc = k_correction(own_c, pc_r.at[0], 2)
    got(h3)
    before, after = coarse_halo(0)

    def store4(v, i, r):
        rst[v, i] = r - rst[v, i]

    every_row = list(range(crows))
    finish(cacc, crows, 2, kc, i_edges(before, after, cs, crows), store4, every_row)
    own_part(c1, racc, crows, 2)
    sub_got(k4)
    kc = k_correction(own_d, pc_r.at[1], 2)
    got(h4)
    before, after = coarse_halo(1)

    def store5(v, i, r):
        change = cst[i] * (r - rst[v, i])
        for ii in (2 * i, 2 * i + 1):
            upd[v, ii] = s2[v, 2 + ii] - change

    finish(racc, crows, 2, kc, i_edges(before, after, c1, crows), store5, every_row)
    for c in (h0, h1, h2, h3, h4):
        sent(c)
    for c in (k0, k1, k2, k3, k4):
        sub_sent(c)


def write_out(upd, res, upd_hbm, res_hbm, sems):
    copies = [
        pltpu.make_async_copy(upd, upd_hbm, sems.at[0]),
        pltpu.make_async_copy(res, res_hbm, sems.at[1]),
    ]
    for c in copies:
        c.start()
    for c in copies:
        c.wait()


def solution(mesh):
    nb, ns = mesh.shape["blk"], mesh.shape["sub"]

    def body(flow_state, timestep, coupling, face_type, face_rot):
        nv, rows, nj, nk = flow_state.shape
        f32 = jnp.float32
        half = rows // 2
        any_spec = pl.BlockSpec(memory_space=pl.ANY)
        vm = lambda *s: pltpu.VMEM(s + (nj, nk), f32)
        out = jax.ShapeDtypeStruct(flow_state.shape, f32)
        held = pltpu.VMEM(flow_state.shape, f32)
        vmem = pl.BlockSpec(memory_space=pltpu.VMEM)
        made = pl.pallas_call(
            functools.partial(kernel, nb, ns),
            out_shape=(held, held),
            in_specs=[any_spec] * 5,
            out_specs=(vmem, vmem),
            scratch_shapes=[
                pltpu.SMEM(coupling.shape, f32),
                pltpu.SMEM(face_type.shape, jnp.int32), pltpu.SMEM(face_rot.shape, jnp.int32),
                vm(nv, rows + 4), vm(nv, rows + 4), vm(nv, rows + 4), vm(rows),
                vm(nv, rows), vm(nv, half), vm(nv, half), vm(nv, half),
                vm(nv, half + 4), vm(nv, half + 4), vm(half),
                vm(3, nv), vm(3, 2, nv), vm(3, 2, nv, 2),
                vm(2, nv), vm(2, 2, nv), vm(2, 2, nv), vm(2, 2, nv),
                pltpu.SemaphoreType.DMA((5,)),
                pltpu.SemaphoreType.DMA((5, 2)), pltpu.SemaphoreType.DMA((5, 2)),
                pltpu.SemaphoreType.DMA((5, 2)), pltpu.SemaphoreType.DMA((5, 2)),
            ],
            compiler_params=pltpu.CompilerParams(collective_id=0, has_side_effects=True),
        )(coupling, face_type, face_rot, flow_state, timestep)
        return pl.pallas_call(
            write_out,
            out_shape=(out, out),
            in_specs=[vmem, vmem],
            out_specs=(any_spec, any_spec),
            scratch_shapes=[pltpu.SemaphoreType.DMA((2,))],
        )(*(pltpu.with_memory_space_constraint(m, pltpu.VMEM) for m in made))

    return jax.shard_map(
        body,
        mesh=mesh,
        in_specs=(
            P(None, "blk", None, "sub"),
            P("blk", None, "sub"),
            P(),
            P("blk", None),
            P("blk", None),
        ),
        out_specs=(P(None, "blk", None, "sub"), P(None, "blk", None, "sub")),
        check_vma=False,
    )
```

```python
import functools

import jax
import jax.numpy as jnp
from jax import lax
from jax.experimental import pallas as pl
from jax.experimental.pallas import tpu as pltpu
from jax.sharding import PartitionSpec as P

NEAR = -0.13
FAR = 0.02
CENTRE = 0.66
FIRST = 0.4
NV = 6


def kernel(
    nb, ns, coup_hbm, ftype_hbm, frot_hbm, q_hbm, dt_hbm, upd, res,
    coup, ftype, frot, q0, s1, s2, dt, acc, cacc, racc, rst, cs, c1, cst,
    pf_s, pf_r, hf_r, pc_s, pc_r, hc_s, hc_r,
    loc, hs_sem, hr_sem, ks_sem, kr_sem,
):
    rows, nj, nk = dt.shape
    crows = rows // 2
    blk, sub = lax.axis_index("blk"), lax.axis_index("sub")
    nxt, prv = lax.rem(blk + 1, nb), lax.rem(blk + nb - 1, nb)
    right, left = lax.rem(sub + 1, ns), lax.rem(sub + ns - 1, ns)
    has_left, has_right = sub > 0, sub < ns - 1

    load_q = pltpu.make_async_copy(q_hbm, q0.at[:, pl.ds(2, rows)], loc.at[0])
    load_t = pltpu.make_async_copy(dt_hbm, dt, loc.at[1])
    loads = [load_q, load_t]
    for n, (src, dst) in enumerate(((coup_hbm, coup), (ftype_hbm, ftype), (frot_hbm, frot))):
        loads.append(pltpu.make_async_copy(src, dst, loc.at[2 + n]))

    barrier = pltpu.get_barrier_semaphore()
    pl.semaphore_signal(barrier, inc=1, device_id={"blk": nxt})
    pl.semaphore_signal(barrier, inc=1, device_id={"blk": prv})

    @pl.when(has_left)
    def _():
        pl.semaphore_signal(barrier, inc=1, device_id={"sub": left})

    @pl.when(has_right)
    def _():
        pl.semaphore_signal(barrier, inc=1, device_id={"sub": right})

    for load in loads:
        load.start()

    shape = (nj, nk)
    jj = lax.broadcasted_iota(jnp.int32, shape, 0)
    kk = lax.broadcasted_iota(jnp.int32, shape, 1)

    def splat(ref, side):
        return jnp.full(shape, ref[0, side], jnp.int32)


    def hcoup(d, u, v):
        return 0.5 * coup[d, u, v]

    def half_flux(x, d):
        s = 0.25 * x[1 + d]
        out = []
        for u in range(NV):
            total = s * x[u]
            for v in range(NV):
                total = total + hcoup(d, u, v) * x[v]
            out.append(total)
        return out

    def roll(x, shift, axis):
        return pltpu.roll(x, shift % x.shape[axis], axis)

    def zero_ends(ref, n):
        for v in range(NV):
            for i in (0, 1, n + 2, n + 3):
                ref[v, i] = jnp.zeros(shape, jnp.float32)

    def own_part(ref, out, n, h):
        step = 2
        j3 = lax.broadcasted_iota(jnp.int32, (step, nj, nk), 1)

        def row(t, carry):
            i0 = t * step

            def at(v, off):
                return ref[v, pl.ds(i0 + 2 + off, step)]

            q = [at(v, 0) for v in range(NV)]
            damp, diffs, sides = [], [], []
            ip = [at(v, 1) for v in range(NV)]
            im = [at(v, -1) for v in range(NV)]
            kp = [roll(x, -h, 2) for x in q]
            km = [roll(x, h, 2) for x in q]
            rp = [roll(x, -h, 1) for x in q]
            rm = [roll(x, h, 1) for x in q]
            jp, jm = [], []
            for v in range(NV):
                sign = -1.0 if v == 2 else 1.0
                edge = sign * q[v] if v == 2 else q[v]
                jp.append(jnp.where(j3 >= nj - h, edge, rp[v]))
                jm.append(jnp.where(j3 < h, edge, rm[v]))
                swap_hi = jnp.where(j3 < nj - h, rp[v], rm[v])
                swap_lo = jnp.where(j3 < h, rp[v], rm[v])
                if v == 2:
                    swap_hi, swap_lo = -swap_hi, -swap_lo
                jpp = jnp.where(j3 < nj - 2 * h, roll(q[v], -2 * h, 1), swap_hi)
                jmm = jnp.where(j3 >= 2 * h, roll(q[v], 2 * h, 1), swap_lo)
                near = ((ip[v] + im[v]) + (jp[v] + jm[v])) + (kp[v] + km[v])
                far = ((at(v, 2) + at(v, -2)) + (jpp + jmm)) + (
                    roll(q[v], -2 * h, 2) + roll(q[v], 2 * h, 2)
                )
                damp.append(CENTRE * q[v] + NEAR * near + FAR * far)
            for d, (p, m) in enumerate(((ip, im), (jp, jm), (kp, km))):
                sp, sm = 0.25 * p[1 + d], 0.25 * m[1 + d]
                diff = [p[v] - m[v] for v in range(NV)]
                for u in range(NV):
                    total = sp * p[u] - sm * m[u]
                    for v in range(NV):
                        total = total + hcoup(d, u, v) * diff[v]
                    damp[u] = damp[u] + total
            for u in range(NV):
                out[u, pl.ds(i0, step)] = damp[u]
            return carry

        lax.fori_loop(0, n // step, row, 0)

    width = 4 * rows
    per = nk // width

    def pack(ref, dst, n, h):
        group = kk // (4 * h)
        packed = []
        for first in range(0, NV, per):
            p = None
            for v in range(first, min(first + per, NV)):
                for i in range(n):
                    spot = (v - first) * n + i
                    x = roll(ref[v, 2 + i], 2 * h + 4 * h * spot, 1)
                    p = x if p is None else jnp.where(group == spot, x, p)
            dst[first // per] = p
            packed.append(p)
        return packed

    def unpack(packed):
        return [roll(packed[v // per], -(v % per) * width, 1) for v in range(NV)]

    def k_edges(low, high, h):
        r = kk % (4 * h)
        near = [jnp.where(r < 2 * h, low[v], high[v]) for v in range(NV)]
        hf = half_flux(near, 2)
        out = []
        for v in range(NV):
            e = jnp.where(r < 2 * h, -hf[v], hf[v]) + NEAR * near[v]
            far = FAR * jnp.where(r < 2 * h, roll(high[v], -2 * h, 1), roll(low[v], 2 * h, 1))
            inner = jnp.where(r < 2 * h, roll(e, -h, 1), roll(e, h, 1))
            out.append(far + jnp.where((r >= h) & (r < 3 * h), inner, 0.0))
        return out

    def k_correction(own, ref, h):
        count = ref.shape[1]
        low = [jnp.where(jnp.full(shape, sub) > 0, ref[0, n], 0.0) for n in range(count)]
        high = [jnp.where(jnp.full(shape, sub) < ns - 1, ref[1, n], 0.0) for n in range(count)]
        got = k_edges(unpack(low), unpack(high), h)
        return [got[v] - own[v] for v in range(NV)]

    def flip(x):
        bit = 1
        while bit < nj:
            x = jnp.where((jj & bit) == 0, roll(x, -bit, 0), roll(x, bit, 0))
            bit *= 2
        return x

    def ghost(side, same, other, own):
        kind, rot = kinds[side], rots[side]
        out = []
        for v in range(NV):
            wall = -own[v] if v == 1 else own[v]
            g = jnp.where(
                kind == 0, same[v], jnp.where(kind == 1, other[v], jnp.where(kind == 2, wall, 0.0))
            )
            out.append(jnp.where((rot & 1) == 1, flip(g), g))
        turn = ((rot >> 1) & 1) == 1
        out[2], out[3] = jnp.where(turn, -out[3], out[2]), jnp.where(turn, out[2], out[3])
        return out

    def i_edges(before, after, ref, n):
        own = lambda i: [ref[v, 2 + i] for v in range(NV)]
        lo_near = ghost(0, before[1], after[0], own(0))
        lo_far = ghost(0, before[0], after[1], own(1))
        hi_near = ghost(1, after[0], before[1], own(n - 1))
        hi_far = ghost(1, after[1], before[0], own(n - 2))
        lo_f, hi_f = half_flux(lo_near, 0), half_flux(hi_near, 0)
        each = range(NV)
        return {
            0: [FAR * lo_far[v] + NEAR * lo_near[v] - lo_f[v] for v in each],
            1: [FAR * lo_near[v] for v in each],
            n - 1: [FAR * hi_far[v] + NEAR * hi_near[v] + hi_f[v] for v in each],
            n - 2: [FAR * hi_near[v] for v in each],
        }

    def finish(out, n, h, kc, edges, then, order):
        mask = (kk < 2 * h) | (kk >= nk - 2 * h)
        for i in order:
            for v in range(NV):
                r = out[v, i] + jnp.where(mask, roll(kc[v], -(2 * h + 4 * h * i), 1), 0.0)
                if i in edges:
                    r = r + edges[i][v]
                then(v, i, r)

    def pair_sum(x):
        x = x + jnp.where((kk & 1) == 0, roll(x, -1, 1), roll(x, 1, 1))
        return x + jnp.where((jj & 1) == 0, roll(x, -1, 0), roll(x, 1, 0))

    def blk_copies(number, to_next, to_prev, dst):
        made = []
        for side, (src, who) in enumerate(((to_next, nxt), (to_prev, prv))):
            made.append(
                pltpu.make_async_remote_copy(
                    src_ref=src, dst_ref=dst.at[side],
                    send_sem=hs_sem.at[number, side], recv_sem=hr_sem.at[number, side],
                    device_id={"blk": who},
                )
            )
        return made

    def sub_copies(number, src, dst):
        made = []
        for side, who in enumerate((right, left)):
            made.append(
                pltpu.make_async_remote_copy(
                    src_ref=src, dst_ref=dst.at[side],
                    send_sem=ks_sem.at[number, side], recv_sem=kr_sem.at[number, side],
                    device_id={"sub": who},
                )
            )
        return made

    def go(copies):
        for c in copies:
            c.start()

    def sub_go(copies):
        pl.when(has_right)(copies[0].start)
        pl.when(has_left)(copies[1].start)

    def got(copies):
        for c in copies:
            c.wait_recv()

    def sub_got(copies):
        pl.when(has_left)(copies[0].wait_recv)
        pl.when(has_right)(copies[1].wait_recv)

    def sent(copies):
        for c in copies:
            c.wait_send()

    def sub_sent(copies):
        pl.when(has_right)(copies[0].wait_send)
        pl.when(has_left)(copies[1].wait_send)

    def fine_halo(number):
        read = lambda side: [[hf_r[number, side, v, r] for v in range(NV)] for r in (0, 1)]
        return read(0), read(1)

    def coarse_halo(number):
        def read(side):
            x = [hc_r[number, side, v] for v in range(NV)]
            even = (jj & 1) == 0
            return [
                [jnp.where(even, y, roll(y, 1, 0)) for y in x],
                [jnp.where(even, roll(y, -1, 0), y) for y in x],
            ]
        return read(0), read(1)

    def coarse_rows(number, ref):
        even = (jj & 1) == 0
        for v in range(NV):
            hc_s[number, 0, v] = jnp.where(even, ref[v, crows], ref[v, crows + 1])
            hc_s[number, 1, v] = jnp.where(even, ref[v, 2], ref[v, 3])

    edge_first = [0, 1, rows - 2, rows - 1] + list(range(2, rows - 2))
    every = []

    zero_ends(q0, rows)
    zero_ends(s1, rows)
    zero_ends(s2, rows)
    zero_ends(cs, crows)
    zero_ends(c1, crows)
    ends = jnp.where(has_left, 0, 1) + jnp.where(has_right, 0, 1)
    load_q.wait()
    pl.semaphore_wait(barrier, 4 - ends)
    h0 = blk_copies(0, q0.at[:, pl.ds(rows, 2)], q0.at[:, pl.ds(2, 2)], hf_r.at[0])
    go(h0)
    for load in loads[1:]:
        load.wait()
    kinds = [splat(ftype, side) for side in (0, 1)]
    rots = [splat(frot, side) for side in (0, 1)]
    packed = pack(q0, pf_s.at[0], rows, 1)
    k0 = sub_copies(0, pf_s.at[0], pf_r.at[0])
    sub_go(k0)
    own = k_edges(*[unpack(packed)] * 2, 1)
    own_part(q0, acc, rows, 1)
    for i in range(crows):
        cst[i] = 0.125 * pair_sum(dt[2 * i] + dt[2 * i + 1])
    sub_got(k0)
    kc = k_correction(own, pf_r.at[0], 1)
    got(h0)
    before, after = fine_halo(0)

    def store1(v, i, r):
        s1[v, 2 + i] = q0[v, 2 + i] - FIRST * dt[i] * r

    finish(acc, rows, 1, kc, i_edges(before, after, q0, rows), store1, edge_first)

    h1 = blk_copies(1, s1.at[:, pl.ds(rows, 2)], s1.at[:, pl.ds(2, 2)], hf_r.at[1])
    go(h1)
    packed = pack(s1, pf_s.at[1], rows, 1)
    k1 = sub_copies(1, pf_s.at[1], pf_r.at[1])
    sub_go(k1)
    own = k_edges(*[unpack(packed)] * 2, 1)
    own_part(s1, acc, rows, 1)
    sub_got(k1)
    kc = k_correction(own, pf_r.at[1], 1)
    got(h1)
    before, after = fine_halo(1)

    def store2(v, i, r):
        s2[v, 2 + i] = q0[v, 2 + i] - dt[i] * r

    finish(acc, rows, 1, kc, i_edges(before, after, s1, rows), store2, edge_first)

    h2 = blk_copies(2, s2.at[:, pl.ds(rows, 2)], s2.at[:, pl.ds(2, 2)], hf_r.at[2])
    go(h2)
    packed = pack(s2, pf_s.at[2], rows, 1)
    k2 = sub_copies(2, pf_s.at[2], pf_r.at[2])
    sub_go(k2)
    own = k_edges(*[unpack(packed)] * 2, 1)
    for v in range(NV):
        for i in range(crows):
            cs[v, 2 + i] = 0.125 * pair_sum(s2[v, 2 + 2 * i] + s2[v, 3 + 2 * i])
    coarse_rows(0, cs)
    h3 = blk_copies(3, hc_s.at[0, 0], hc_s.at[0, 1], hc_r.at[0])
    go(h3)
    packed = pack(cs, pc_s.at[0], crows, 2)
    k3 = sub_copies(3, pc_s.at[0], pc_r.at[0])
    sub_go(k3)
    own_c = k_edges(*[unpack(packed)] * 2, 2)
    own_part(s2, acc, rows, 1)
    sub_got(k2)
    kc = k_correction(own, pf_r.at[2], 1)
    got(h2)
    before, after = fine_halo(2)

    def store3(v, i, r):
        res[v, i] = r

    finish(acc, rows, 1, kc, i_edges(before, after, s2, rows), store3, edge_first)
    for v in range(NV):
        for i in range(crows):
            r = 0.125 * pair_sum(res[v, 2 * i] + res[v, 2 * i + 1])
            rst[v, i] = r
            c1[v, 2 + i] = cs[v, 2 + i] - FIRST * cst[i] * r

    coarse_rows(1, c1)
    h4 = blk_copies(4, hc_s.at[1, 0], hc_s.at[1, 1], hc_r.at[1])
    go(h4)
    packed = pack(c1, pc_s.at[1], crows, 2)
    k4 = sub_copies(4, pc_s.at[1], pc_r.at[1])
    sub_go(k4)
    own_d = k_edges(*[unpack(packed)] * 2, 2)
    own_part(cs, cacc, crows, 2)
    sub_got(k3)
    kc = k_correction(own_c, pc_r.at[0], 2)
    got(h3)
    before, after = coarse_halo(0)

    def store4(v, i, r):
        rst[v, i] = r - rst[v, i]

    every_row = list(range(crows))
    finish(cacc, crows, 2, kc, i_edges(before, after, cs, crows), store4, every_row)
    own_part(c1, racc, crows, 2)
    sub_got(k4)
    kc = k_correction(own_d, pc_r.at[1], 2)
    got(h4)
    before, after = coarse_halo(1)

    def store5(v, i, r):
        change = cst[i] * (r - rst[v, i])
        for ii in (2 * i, 2 * i + 1):
            upd[v, ii] = s2[v, 2 + ii] - change

    finish(racc, crows, 2, kc, i_edges(before, after, c1, crows), store5, every_row)
    for c in (h0, h1, h2, h3, h4):
        sent(c)
    for c in (k0, k1, k2, k3, k4):
        sub_sent(c)


def write_out(upd, res, upd_hbm, res_hbm, sems):
    copies = [
        pltpu.make_async_copy(upd, upd_hbm, sems.at[0]),
        pltpu.make_async_copy(res, res_hbm, sems.at[1]),
    ]
    for c in copies:
        c.start()
    for c in copies:
        c.wait()


def solution(mesh):
    nb, ns = mesh.shape["blk"], mesh.shape["sub"]

    def body(flow_state, timestep, coupling, face_type, face_rot):
        nv, rows, nj, nk = flow_state.shape
        f32 = jnp.float32
        half = rows // 2
        ends = -(-nv // (nk // (4 * rows)))
        any_spec = pl.BlockSpec(memory_space=pl.ANY)
        vm = lambda *s: pltpu.VMEM(s + (nj, nk), f32)
        out = jax.ShapeDtypeStruct(flow_state.shape, f32)
        held = pltpu.VMEM(flow_state.shape, f32)
        vmem = pl.BlockSpec(memory_space=pltpu.VMEM)
        made = pl.pallas_call(
            functools.partial(kernel, nb, ns),
            out_shape=(held, held),
            in_specs=[any_spec] * 5,
            out_specs=(vmem, vmem),
            scratch_shapes=[
                pltpu.SMEM(coupling.shape, f32),
                pltpu.SMEM(face_type.shape, jnp.int32), pltpu.SMEM(face_rot.shape, jnp.int32),
                vm(nv, rows + 4), vm(nv, rows + 4), vm(nv, rows + 4), vm(rows),
                vm(nv, rows), vm(nv, half), vm(nv, half), vm(nv, half),
                vm(nv, half + 4), vm(nv, half + 4), vm(half),
                vm(3, ends), vm(3, 2, ends), vm(3, 2, nv, 2),
                vm(2, ends), vm(2, 2, ends), vm(2, 2, nv), vm(2, 2, nv),
                pltpu.SemaphoreType.DMA((5,)),
                pltpu.SemaphoreType.DMA((5, 2)), pltpu.SemaphoreType.DMA((5, 2)),
                pltpu.SemaphoreType.DMA((5, 2)), pltpu.SemaphoreType.DMA((5, 2)),
            ],
            compiler_params=pltpu.CompilerParams(collective_id=0, has_side_effects=True),
        )(coupling, face_type, face_rot, flow_state, timestep)
        return pl.pallas_call(
            write_out,
            out_shape=(out, out),
            in_specs=[vmem, vmem],
            out_specs=(any_spec, any_spec),
            scratch_shapes=[pltpu.SemaphoreType.DMA((2,))],
        )(*(pltpu.with_memory_space_constraint(m, pltpu.VMEM) for m in made))

    return jax.shard_map(
        body,
        mesh=mesh,
        in_specs=(
            P(None, "blk", None, "sub"),
            P("blk", None, "sub"),
            P(),
            P("blk", None),
            P("blk", None),
        ),
        out_specs=(P(None, "blk", None, "sub"), P(None, "blk", None, "sub")),
        check_vma=False,
    )
```

```python
import functools

import jax
import jax.numpy as jnp
from jax import lax
from jax.experimental import pallas as pl
from jax.experimental.pallas import tpu as pltpu
from jax.sharding import PartitionSpec as P

NEAR = -0.13
FAR = 0.02
CENTRE = 0.66
FIRST = 0.4
NV = 6


def kernel(
    nb, ns, coup_hbm, ftype_hbm, frot_hbm, q_hbm, dt_hbm, upd, res,
    coup, ftype, frot, q0, s1, s2, dt, acc, cacc, racc, rst, cs, c1, cst,
    pf_s, pf_r, hf_r, pc_s, pc_r, hc_s, hc_r,
    loc, hs_sem, hr_sem, ks_sem, kr_sem,
):
    rows, nj, nk = dt.shape
    crows = rows // 2
    blk, sub = lax.axis_index("blk"), lax.axis_index("sub")
    nxt, prv = lax.rem(blk + 1, nb), lax.rem(blk + nb - 1, nb)
    right, left = lax.rem(sub + 1, ns), lax.rem(sub + ns - 1, ns)
    has_left, has_right = sub > 0, sub < ns - 1

    load_q = pltpu.make_async_copy(q_hbm, q0.at[:, pl.ds(2, rows)], loc.at[0])
    load_t = pltpu.make_async_copy(dt_hbm, dt, loc.at[1])
    loads = [load_q, load_t]
    for n, (src, dst) in enumerate(((coup_hbm, coup), (ftype_hbm, ftype), (frot_hbm, frot))):
        loads.append(pltpu.make_async_copy(src, dst, loc.at[2 + n]))

    barrier = pltpu.get_barrier_semaphore()
    pl.semaphore_signal(barrier, inc=1, device_id={"blk": nxt})
    pl.semaphore_signal(barrier, inc=1, device_id={"blk": prv})

    @pl.when(has_left)
    def _():
        pl.semaphore_signal(barrier, inc=1, device_id={"sub": left})

    @pl.when(has_right)
    def _():
        pl.semaphore_signal(barrier, inc=1, device_id={"sub": right})

    for load in loads:
        load.start()

    shape = (nj, nk)
    jj = lax.broadcasted_iota(jnp.int32, shape, 0)
    kk = lax.broadcasted_iota(jnp.int32, shape, 1)

    def splat(ref, side):
        return jnp.full(shape, ref[0, side], jnp.int32)


    def hcoup(d, u, v):
        return 0.5 * coup[d, u, v]

    def half_flux(x, d):
        s = 0.25 * x[1 + d]
        out = []
        for u in range(NV):
            total = s * x[u]
            for v in range(NV):
                total = total + hcoup(d, u, v) * x[v]
            out.append(total)
        return out

    def roll(x, shift, axis):
        return pltpu.roll(x, shift % x.shape[axis], axis)

    def zero_ends(ref, n):
        for v in range(NV):
            for i in (0, 1, n + 2, n + 3):
                ref[v, i] = jnp.zeros(shape, jnp.float32)

    def own_part(ref, out, n, h):
        step = 2
        j3 = lax.broadcasted_iota(jnp.int32, (step, nj, nk), 1)

        def row(t, carry):
            i0 = t * step

            def at(v, off):
                return ref[v, pl.ds(i0 + 2 + off, step)]

            q = [at(v, 0) for v in range(NV)]
            damp, diffs, sides = [], [], []
            ip = [at(v, 1) for v in range(NV)]
            im = [at(v, -1) for v in range(NV)]
            kp = [roll(x, -h, 2) for x in q]
            km = [roll(x, h, 2) for x in q]
            rp = [roll(x, -h, 1) for x in q]
            rm = [roll(x, h, 1) for x in q]
            jp, jm = [], []
            for v in range(NV):
                sign = -1.0 if v == 2 else 1.0
                edge = sign * q[v] if v == 2 else q[v]
                jp.append(jnp.where(j3 >= nj - h, edge, rp[v]))
                jm.append(jnp.where(j3 < h, edge, rm[v]))
                swap_hi = jnp.where(j3 < nj - h, rp[v], rm[v])
                swap_lo = jnp.where(j3 < h, rp[v], rm[v])
                if v == 2:
                    swap_hi, swap_lo = -swap_hi, -swap_lo
                jpp = jnp.where(j3 < nj - 2 * h, roll(q[v], -2 * h, 1), swap_hi)
                jmm = jnp.where(j3 >= 2 * h, roll(q[v], 2 * h, 1), swap_lo)
                near = ((ip[v] + im[v]) + (jp[v] + jm[v])) + (kp[v] + km[v])
                far = ((at(v, 2) + at(v, -2)) + (jpp + jmm)) + (
                    roll(q[v], -2 * h, 2) + roll(q[v], 2 * h, 2)
                )
                damp.append(CENTRE * q[v] + NEAR * near + FAR * far)
            for d, (p, m) in enumerate(((ip, im), (jp, jm), (kp, km))):
                sp, sm = 0.25 * p[1 + d], 0.25 * m[1 + d]
                diff = [p[v] - m[v] for v in range(NV)]
                for u in range(NV):
                    total = sp * p[u] - sm * m[u]
                    for v in range(NV):
                        total = total + hcoup(d, u, v) * diff[v]
                    damp[u] = damp[u] + total
            for u in range(NV):
                out[u, pl.ds(i0, step)] = damp[u]
            return carry

        lax.fori_loop(0, n // step, row, 0)

    width = 4 * rows
    per = nk // width

    def pack(ref, dst, n, h):
        group = kk // (4 * h)
        packed = []
        for first in range(0, NV, per):
            p = None
            for v in range(first, min(first + per, NV)):
                for i in range(n):
                    spot = (v - first) * n + i
                    x = roll(ref[v, 2 + i], 2 * h + 4 * h * spot, 1)
                    p = x if p is None else jnp.where(group == spot, x, p)
            dst[first // per] = p
            packed.append(p)
        return packed

    def unpack(packed):
        return [roll(packed[v // per], -(v % per) * width, 1) for v in range(NV)]

    def k_edges(low, high, h):
        r = kk % (4 * h)
        near = [jnp.where(r < 2 * h, low[v], high[v]) for v in range(NV)]
        hf = half_flux(near, 2)
        out = []
        for v in range(NV):
            e = jnp.where(r < 2 * h, -hf[v], hf[v]) + NEAR * near[v]
            far = FAR * jnp.where(r < 2 * h, roll(high[v], -2 * h, 1), roll(low[v], 2 * h, 1))
            inner = jnp.where(r < 2 * h, roll(e, -h, 1), roll(e, h, 1))
            out.append(far + jnp.where((r >= h) & (r < 3 * h), inner, 0.0))
        return out

    def k_correction(own, ref, h):
        count = ref.shape[1]
        low = [jnp.where(jnp.full(shape, sub) > 0, ref[0, n], 0.0) for n in range(count)]
        high = [jnp.where(jnp.full(shape, sub) < ns - 1, ref[1, n], 0.0) for n in range(count)]
        got = k_edges(unpack(low), unpack(high), h)
        return [got[v] - own[v] for v in range(NV)]

    def flip(x):
        bit = 1
        while bit < nj:
            x = jnp.where((jj & bit) == 0, roll(x, -bit, 0), roll(x, bit, 0))
            bit *= 2
        return x

    def ghost(side, same, other, own):
        kind, rot = kinds[side], rots[side]
        out = []
        for v in range(NV):
            wall = -own[v] if v == 1 else own[v]
            g = jnp.where(
                kind == 0, same[v], jnp.where(kind == 1, other[v], jnp.where(kind == 2, wall, 0.0))
            )
            out.append(jnp.where((rot & 1) == 1, flip(g), g))
        turn = ((rot >> 1) & 1) == 1
        out[2], out[3] = jnp.where(turn, -out[3], out[2]), jnp.where(turn, out[2], out[3])
        return out

    def i_edges(before, after, ref, n):
        own = lambda i: [ref[v, 2 + i] for v in range(NV)]
        lo_near = ghost(0, before[1], after[0], own(0))
        lo_far = ghost(0, before[0], after[1], own(1))
        hi_near = ghost(1, after[0], before[1], own(n - 1))
        hi_far = ghost(1, after[1], before[0], own(n - 2))
        lo_f, hi_f = half_flux(lo_near, 0), half_flux(hi_near, 0)
        each = range(NV)
        return {
            0: [FAR * lo_far[v] + NEAR * lo_near[v] - lo_f[v] for v in each],
            1: [FAR * lo_near[v] for v in each],
            n - 1: [FAR * hi_far[v] + NEAR * hi_near[v] + hi_f[v] for v in each],
            n - 2: [FAR * hi_near[v] for v in each],
        }

    def finish(out, n, h, kc, edges, then, order):
        mask = (kk < 2 * h) | (kk >= nk - 2 * h)
        for i in order:
            for v in range(NV):
                r = out[v, i] + jnp.where(mask, roll(kc[v], -(2 * h + 4 * h * i), 1), 0.0)
                if i in edges:
                    r = r + edges[i][v]
                then(v, i, r)

    def pair_sum(x):
        x = x + jnp.where((kk & 1) == 0, roll(x, -1, 1), roll(x, 1, 1))
        return x + jnp.where((jj & 1) == 0, roll(x, -1, 0), roll(x, 1, 0))

    def blk_copies(number, to_next, to_prev, dst):
        made = []
        for side, (src, who) in enumerate(((to_next, nxt), (to_prev, prv))):
            made.append(
                pltpu.make_async_remote_copy(
                    src_ref=src, dst_ref=dst.at[side],
                    send_sem=hs_sem.at[number, side], recv_sem=hr_sem.at[number, side],
                    device_id={"blk": who},
                )
            )
        return made

    def sub_copies(number, src, dst):
        made = []
        for side, who in enumerate((right, left)):
            made.append(
                pltpu.make_async_remote_copy(
                    src_ref=src, dst_ref=dst.at[side],
                    send_sem=ks_sem.at[number, side], recv_sem=kr_sem.at[number, side],
                    device_id={"sub": who},
                )
            )
        return made

    def go(copies):
        for c in copies:
            c.start()

    def sub_go(copies):
        pl.when(has_right)(copies[0].start)
        pl.when(has_left)(copies[1].start)

    def got(copies):
        for c in copies:
            c.wait_recv()

    def sub_got(copies):
        pl.when(has_left)(copies[0].wait_recv)
        pl.when(has_right)(copies[1].wait_recv)

    def sent(copies):
        for c in copies:
            c.wait_send()

    def sub_sent(copies):
        pl.when(has_right)(copies[0].wait_send)
        pl.when(has_left)(copies[1].wait_send)

    def fine_halo(number):
        read = lambda side: [[hf_r[number, side, v, r] for v in range(NV)] for r in (0, 1)]
        return read(0), read(1)

    def coarse_halo(number):
        def read(side):
            x = [hc_r[number, side, v] for v in range(NV)]
            even = (jj & 1) == 0
            return [
                [jnp.where(even, y, roll(y, 1, 0)) for y in x],
                [jnp.where(even, roll(y, -1, 0), y) for y in x],
            ]
        return read(0), read(1)

    def coarse_rows(number, ref):
        even = (jj & 1) == 0
        for v in range(NV):
            hc_s[number, 0, v] = jnp.where(even, ref[v, crows], ref[v, crows + 1])
            hc_s[number, 1, v] = jnp.where(even, ref[v, 2], ref[v, 3])

    edge_first = [0, 1, rows - 2, rows - 1] + list(range(2, rows - 2))
    every = []

    zero_ends(q0, rows)
    zero_ends(s1, rows)
    zero_ends(s2, rows)
    zero_ends(cs, crows)
    zero_ends(c1, crows)
    ends = jnp.where(has_left, 0, 1) + jnp.where(has_right, 0, 1)
    load_q.wait()
    pl.semaphore_wait(barrier, 4 - ends)
    h0 = blk_copies(0, q0.at[:, pl.ds(rows, 2)], q0.at[:, pl.ds(2, 2)], hf_r.at[0])
    go(h0)
    for load in loads[1:]:
        load.wait()
    kinds = [splat(ftype, side) for side in (0, 1)]
    rots = [splat(frot, side) for side in (0, 1)]
    packed = pack(q0, pf_s.at[0], rows, 1)
    k0 = sub_copies(0, pf_s.at[0], pf_r.at[0])
    sub_go(k0)
    own = k_edges(*[unpack(packed)] * 2, 1)
    own_part(q0, acc, rows, 1)
    for i in range(crows):
        cst[i] = 0.125 * pair_sum(dt[2 * i] + dt[2 * i + 1])
    sub_got(k0)
    kc = k_correction(own, pf_r.at[0], 1)
    got(h0)
    before, after = fine_halo(0)

    def store1(v, i, r):
        s1[v, 2 + i] = q0[v, 2 + i] - FIRST * dt[i] * r

    edges = i_edges(before, after, q0, rows)
    finish(acc, rows, 1, kc, edges, store1, edge_first[:4])
    h1 = blk_copies(1, s1.at[:, pl.ds(rows, 2)], s1.at[:, pl.ds(2, 2)], hf_r.at[1])
    go(h1)
    finish(acc, rows, 1, kc, edges, store1, edge_first[4:])

    packed = pack(s1, pf_s.at[1], rows, 1)
    k1 = sub_copies(1, pf_s.at[1], pf_r.at[1])
    sub_go(k1)
    own = k_edges(*[unpack(packed)] * 2, 1)
    own_part(s1, acc, rows, 1)
    sub_got(k1)
    kc = k_correction(own, pf_r.at[1], 1)
    got(h1)
    before, after = fine_halo(1)

    def store2(v, i, r):
        s2[v, 2 + i] = q0[v, 2 + i] - dt[i] * r

    edges = i_edges(before, after, s1, rows)
    finish(acc, rows, 1, kc, edges, store2, edge_first[:4])
    h2 = blk_copies(2, s2.at[:, pl.ds(rows, 2)], s2.at[:, pl.ds(2, 2)], hf_r.at[2])
    go(h2)
    finish(acc, rows, 1, kc, edges, store2, edge_first[4:])

    packed = pack(s2, pf_s.at[2], rows, 1)
    k2 = sub_copies(2, pf_s.at[2], pf_r.at[2])
    sub_go(k2)
    own = k_edges(*[unpack(packed)] * 2, 1)
    for v in range(NV):
        for i in range(crows):
            cs[v, 2 + i] = 0.125 * pair_sum(s2[v, 2 + 2 * i] + s2[v, 3 + 2 * i])
    coarse_rows(0, cs)
    h3 = blk_copies(3, hc_s.at[0, 0], hc_s.at[0, 1], hc_r.at[0])
    go(h3)
    packed = pack(cs, pc_s.at[0], crows, 2)
    k3 = sub_copies(3, pc_s.at[0], pc_r.at[0])
    sub_go(k3)
    own_c = k_edges(*[unpack(packed)] * 2, 2)
    own_part(s2, acc, rows, 1)
    sub_got(k2)
    kc = k_correction(own, pf_r.at[2], 1)
    got(h2)
    before, after = fine_halo(2)

    def store3(v, i, r):
        res[v, i] = r

    finish(acc, rows, 1, kc, i_edges(before, after, s2, rows), store3, edge_first)
    for v in range(NV):
        for i in range(crows):
            r = 0.125 * pair_sum(res[v, 2 * i] + res[v, 2 * i + 1])
            rst[v, i] = r
            c1[v, 2 + i] = cs[v, 2 + i] - FIRST * cst[i] * r

    coarse_rows(1, c1)
    h4 = blk_copies(4, hc_s.at[1, 0], hc_s.at[1, 1], hc_r.at[1])
    go(h4)
    packed = pack(c1, pc_s.at[1], crows, 2)
    k4 = sub_copies(4, pc_s.at[1], pc_r.at[1])
    sub_go(k4)
    own_d = k_edges(*[unpack(packed)] * 2, 2)
    own_part(cs, cacc, crows, 2)
    sub_got(k3)
    kc = k_correction(own_c, pc_r.at[0], 2)
    got(h3)
    before, after = coarse_halo(0)

    def store4(v, i, r):
        rst[v, i] = r - rst[v, i]

    every_row = list(range(crows))
    finish(cacc, crows, 2, kc, i_edges(before, after, cs, crows), store4, every_row)
    own_part(c1, racc, crows, 2)
    sub_got(k4)
    kc = k_correction(own_d, pc_r.at[1], 2)
    got(h4)
    before, after = coarse_halo(1)

    def store5(v, i, r):
        change = cst[i] * (r - rst[v, i])
        for ii in (2 * i, 2 * i + 1):
            upd[v, ii] = s2[v, 2 + ii] - change

    finish(racc, crows, 2, kc, i_edges(before, after, c1, crows), store5, every_row)
    for c in (h0, h1, h2, h3, h4):
        sent(c)
    for c in (k0, k1, k2, k3, k4):
        sub_sent(c)


def write_out(upd, res, upd_hbm, res_hbm, sems):
    copies = [
        pltpu.make_async_copy(upd, upd_hbm, sems.at[0]),
        pltpu.make_async_copy(res, res_hbm, sems.at[1]),
    ]
    for c in copies:
        c.start()
    for c in copies:
        c.wait()


def solution(mesh):
    nb, ns = mesh.shape["blk"], mesh.shape["sub"]

    def body(flow_state, timestep, coupling, face_type, face_rot):
        nv, rows, nj, nk = flow_state.shape
        f32 = jnp.float32
        half = rows // 2
        ends = -(-nv // (nk // (4 * rows)))
        any_spec = pl.BlockSpec(memory_space=pl.ANY)
        vm = lambda *s: pltpu.VMEM(s + (nj, nk), f32)
        out = jax.ShapeDtypeStruct(flow_state.shape, f32)
        held = pltpu.VMEM(flow_state.shape, f32)
        vmem = pl.BlockSpec(memory_space=pltpu.VMEM)
        made = pl.pallas_call(
            functools.partial(kernel, nb, ns),
            out_shape=(held, held),
            in_specs=[any_spec] * 5,
            out_specs=(vmem, vmem),
            scratch_shapes=[
                pltpu.SMEM(coupling.shape, f32),
                pltpu.SMEM(face_type.shape, jnp.int32), pltpu.SMEM(face_rot.shape, jnp.int32),
                vm(nv, rows + 4), vm(nv, rows + 4), vm(nv, rows + 4), vm(rows),
                vm(nv, rows), vm(nv, half), vm(nv, half), vm(nv, half),
                vm(nv, half + 4), vm(nv, half + 4), vm(half),
                vm(3, ends), vm(3, 2, ends), vm(3, 2, nv, 2),
                vm(2, ends), vm(2, 2, ends), vm(2, 2, nv), vm(2, 2, nv),
                pltpu.SemaphoreType.DMA((5,)),
                pltpu.SemaphoreType.DMA((5, 2)), pltpu.SemaphoreType.DMA((5, 2)),
                pltpu.SemaphoreType.DMA((5, 2)), pltpu.SemaphoreType.DMA((5, 2)),
            ],
            compiler_params=pltpu.CompilerParams(collective_id=0, has_side_effects=True),
        )(coupling, face_type, face_rot, flow_state, timestep)
        return pl.pallas_call(
            write_out,
            out_shape=(out, out),
            in_specs=[vmem, vmem],
            out_specs=(any_spec, any_spec),
            scratch_shapes=[pltpu.SemaphoreType.DMA((2,))],
        )(*(pltpu.with_memory_space_constraint(m, pltpu.VMEM) for m in made))

    return jax.shard_map(
        body,
        mesh=mesh,
        in_specs=(
            P(None, "blk", None, "sub"),
            P("blk", None, "sub"),
            P(),
            P("blk", None),
            P("blk", None),
        ),
        out_specs=(P(None, "blk", None, "sub"), P(None, "blk", None, "sub")),
        check_vma=False,
    )
```
